32 devices in a mesh: scen: 8 (over y, x, core), col: 4 (over z).
Axes of the slice: x: 2, y: 2, z: 4, core: 2. Of those that a mesh axis runs over, the one named last changes fastest.
Arguments:
- tech: bfloat16 [32, 2048, 4096], P('scen', None, 'col'), may hold values from -0.046875 to 0.046875
- recourse: bfloat16 [32, 2048, 1024], P('scen', None, 'col'), may hold values from -0.125 to 0.125
- rhs: float32 [32, 32, 2048], P(None, 'scen'), may hold values from -6 to 6
- cost_first: float32 [4096], P('col'), may hold values from -6 to 6
- cost_second: float32 [32, 1024], P('scen', 'col'), may hold values from -6 to 6
- cone_id: int32 [32, 2048], P('scen'), may hold values from 0 to 127, never falling along the last dimension, each value on 1 to 64 neighbouring positions
Outputs:
- first_section: float32 [32, 4096], P(None, 'col')
- second_section: float32 [32, 32, 1024], P(None, 'scen', 'col')
- slack: float32 [32, 32, 2048], P(None, 'scen', 'col')
- dual: float32 [32, 32, 2048], P(None, 'scen', 'col')
The draws below stay inside these ranges and needn't reach their ends.
Inputs may be any that keep to these rules, and one draw needn't show every extreme that they name: Along the rows of a scenario cone_id never falls; a cone holds 1 to 64 rows.
All inputs are finite; a program needn't handle non-finite values.
Results may differ from the reference program's by a relative error of at most 0.014.
Values may be sent and summed in bfloat16 or wider, within the bound.
A program may use at most 128 MiB of HBM per device.

```python
import math
import jax
import jax.numpy as jnp
import numpy as np
from jax import lax

M = 2048
NX = 4096
NY = 1024
NCONE = 128
CONE_MOST = 64
BATCH = 32
ITERS = 3
CG_STEPS = 3
SCENS = 32


def steps_of(key, shape, cuts, least, top_value):
    def one(dim, parts):
        draws = jax.random.uniform(jax.random.fold_in(jax.random.fold_in(key, 6), dim), (parts,), jnp.float32, least / len(cuts), top_value / len(cuts))
        return jnp.repeat(jnp.exp(draws), shape[dim] // parts).reshape((-1,) + (1,) * (len(shape) - dim - 1))

    gain = one(*cuts[0])
    for cut in cuts[1:]:
        gain = gain * one(*cut)
    return gain


def split_up(count, total, reach, slope):
    loads = [(1 << 20) // math.isqrt(grade ** slope) + 1 for grade in range(2, count + 1)]
    spare, holding = total - reach - (count - 1), [1] * (count - 1)
    while spare > 0:
        candidates = [i for i in range(count - 1) if holding[i] < reach]
        whole, left = sum([loads[i] for i in candidates]), spare
        for i in candidates:
            more = min(reach - holding[i], max(1, left * loads[i] // whole), spare)
            holding[i] = holding[i] + more
            spare = spare - more
    return np.array([reach] + holding)


def uneven_parts(rng, number_of, total, limit, lean):
    if number_of == 2:
        one = jax.random.randint(rng, (), max(1, total - limit), min(limit, total - 1) + 1)
        return jnp.stack([one, total - one])
    tallies = jnp.asarray(split_up(number_of, total, limit, lean), jnp.int32)
    couples = (number_of - 1) // 2
    source_of, receiver = tallies[1:1 + 2 * couples:2], tallies[2:2 + 2 * couples:2]
    room = jnp.minimum(source_of - 1, limit - receiver)
    moved = jax.random.randint(jax.random.fold_in(rng, 1), (couples,), 0, 1 << 20) % (room + 1)
    tallies = tallies.at[1:1 + 2 * couples:2].set(source_of - moved).at[2:2 + 2 * couples:2].set(receiver + moved)
    return tallies[jax.random.permutation(jax.random.fold_in(rng, 2), number_of)]


def bell_draw(key, shape, spread, reach, split=(), dtype=jnp.bfloat16):
    loudness = steps_of(key, shape, split, -0.22, 0.18) if split else 1.0
    entries = jax.random.normal(key, shape, jnp.float32) * spread * loudness
    return jnp.minimum(jnp.maximum(entries, -reach), reach).astype(dtype)


def setup_inputs(seed: int = 0) -> dict:
    key_of = jax.random.split(jax.random.key(seed), 7)
    tech = bell_draw(key_of[0], (SCENS, M, NX), (SCENS * M // 4) ** -0.5, 0.046875, ((0, 8), (2, 4)))
    recourse = bell_draw(key_of[1], (SCENS, M, NY), M ** -0.5, 0.125, ((0, 8), (2, 4)))
    rhs = bell_draw(key_of[2], (BATCH, SCENS, M), 1.0, 6.0, ((1, 8),), jnp.float32)
    cost_first = bell_draw(key_of[3], (NX,), 1.0, 6.0, ((0, 4),), jnp.float32)
    cost_second = bell_draw(key_of[4], (SCENS, NY), 1.0, 6.0, ((0, 8), (1, 4)), jnp.float32)
    cone_id = jax.vmap(lambda own: jnp.searchsorted(jnp.cumsum(uneven_parts(own, NCONE, M, CONE_MOST, 2)), jnp.arange(M), side="right"))(jax.random.split(key_of[5], SCENS)).reshape((SCENS, M)).astype(jnp.int32)
    return dict(tech=tech, recourse=recourse, rhs=rhs, cost_first=cost_first, cost_second=cost_second, cone_id=cone_id)


HIGH = lax.Precision.HIGHEST

def cone_factors(lead, tail):
    norm_tail = jnp.sqrt(tail)
    inside = norm_tail <= lead
    polar = norm_tail <= -lead
    safe = jnp.where(norm_tail > 0.0, norm_tail, 1.0)
    middle = 0.5 * (lead + norm_tail)
    head = jnp.where(inside, lead, jnp.where(polar, 0.0, middle))
    scale = jnp.where(inside, 1.0, jnp.where(polar, 0.0, middle / safe))
    return (head, scale)

def reference(tech, recourse, rhs, cost_first, cost_second, cone_id):
    f32 = jnp.float32
    bf16 = jnp.bfloat16
    batch = rhs.shape[0]
    scen_count = tech.shape[0]
    rows = tech.shape[1]
    rhs_s = jnp.transpose(rhs, (1, 0, 2))
    starts = jnp.concatenate([jnp.ones((scen_count, 1), f32), (cone_id[:, 1:] != cone_id[:, :-1]).astype(f32)], axis=1)
    labels = lax.broadcasted_iota(jnp.int32, (1, 1, NCONE), 2)
    onehot = (cone_id[:, :, None] == labels).astype(f32)
    start_rows = starts[:, None, :]

    def project(values):
        lead = jnp.einsum('sbm,smc->sbc', values * start_rows, onehot, precision=HIGH)
        tail = jnp.einsum('sbm,smc->sbc', values * values * (1.0 - start_rows), onehot, precision=HIGH)
        head, scale = cone_factors(lead, tail)
        head_rows = jnp.einsum('sbc,smc->sbm', head, onehot, precision=HIGH)
        scale_rows = jnp.einsum('sbc,smc->sbm', scale, onehot, precision=HIGH)
        return start_rows * head_rows + (1.0 - start_rows) * values * scale_rows

    def forward(dir_first_bf, dir_second_bf):

        def single(args):
            tech_s, rec_s, dir_s = args
            return jnp.dot(dir_first_bf, tech_s.T, preferred_element_type=f32) + jnp.dot(dir_s, rec_s.T, preferred_element_type=f32)
        return lax.map(single, (tech, recourse, dir_second_bf))

    def adjoint(rows_bf):

        def single(carry, args):
            tech_s, rec_s, rows_s = args
            return (carry + jnp.dot(rows_s, tech_s, preferred_element_type=f32), jnp.dot(rows_s, rec_s, preferred_element_type=f32))
        return lax.scan(single, jnp.zeros((batch, tech.shape[2]), f32), (tech, recourse, rows_bf))

    def squares(first_vec, second_vec):
        return lax.optimization_barrier(jnp.sum(first_vec * first_vec, axis=1)) + lax.optimization_barrier(jnp.sum(second_vec * second_vec, axis=(0, 2)))
    first_sol = jnp.zeros((batch, tech.shape[2]), f32)
    second_sol = jnp.zeros((scen_count, batch, recourse.shape[2]), f32)
    slack = jnp.zeros((scen_count, batch, rows), f32)
    dual = jnp.zeros((scen_count, batch, rows), f32)
    image = jnp.zeros((scen_count, batch, rows), f32)
    for outer in range(ITERS):
        resid_rows = (rhs_s - slack - dual - image).astype(bf16)
        back_first, back_second = adjoint(resid_rows)
        res_first = back_first - cost_first[None, :]
        res_second = back_second - cost_second[:, None, :]
        res_norm = squares(res_first, res_second)
        dir_first, dir_second = (res_first, res_second)
        for step in range(CG_STEPS):
            image_step = forward(dir_first.astype(bf16), dir_second.astype(bf16))
            curv = squares(dir_first, dir_second) + lax.optimization_barrier(jnp.sum(image_step * image_step, axis=(0, 2)))
            alpha = res_norm / curv
            first_sol = first_sol + alpha[:, None] * dir_first
            second_sol = second_sol + alpha[None, :, None] * dir_second
            image = image + alpha[None, :, None] * image_step
            if step + 1 < CG_STEPS:
                back_first, back_second = adjoint(image_step.astype(bf16))
                res_first = res_first - alpha[:, None] * (dir_first + back_first)
                res_second = res_second - alpha[None, :, None] * (dir_second + back_second)
                new_norm = squares(res_first, res_second)
                ratio = new_norm / res_norm
                dir_first = res_first + ratio[:, None] * dir_first
                dir_second = res_second + ratio[None, :, None] * dir_second
                res_norm = new_norm
        slack = project(rhs_s - image - dual)
        dual = dual + image + slack - rhs_s
    return (first_sol, jnp.transpose(second_sol, (1, 0, 2)), jnp.transpose(slack, (1, 0, 2)), jnp.transpose(dual, (1, 0, 2)))
```

```python
import functools

import jax
import jax.numpy as jnp
from jax import lax
from jax.experimental import pallas as pl
from jax.experimental.pallas import tpu as pltpu
from jax.sharding import PartitionSpec as P

NCONE = 128
ITERS = 3
CG_STEPS = 3


HIGH = lax.Precision.HIGHEST


def cone_factors(lead, tail):
    norm_tail = jnp.sqrt(tail)
    inside = norm_tail <= lead
    polar = norm_tail <= -lead
    safe = jnp.where(norm_tail > 0.0, norm_tail, 1.0)
    middle = 0.5 * (lead + norm_tail)
    head = jnp.where(inside, lead, jnp.where(polar, 0.0, middle))
    scale = jnp.where(inside, 1.0, jnp.where(polar, 0.0, middle / safe))
    return (head, scale)


def body(tech, recourse, rhs, cost_first, cost_second, cone_id):
    f32 = jnp.float32
    bf16 = jnp.bfloat16
    n_scen = lax.axis_size("scen")
    n_col = lax.axis_size("col")
    batch = rhs.shape[0]
    scen_local = tech.shape[0]
    rows = tech.shape[1]
    first_cols = tech.shape[2]
    tech_flat = tech.reshape(scen_local * rows, first_cols)
    starts = jnp.concatenate(
        [jnp.ones((scen_local, 1), f32), (cone_id[:, 1:] != cone_id[:, :-1]).astype(f32)], axis=1
    )
    labels = lax.broadcasted_iota(jnp.int32, (1, 1, NCONE), 2)
    onehot = (cone_id[:, :, None] == labels).astype(f32)
    part_rows = rows // n_col
    row_start = lax.axis_index("col") * part_rows
    row_weight = 1.0 / n_col
    share_cols = first_cols // n_scen
    cost_here = lax.dynamic_slice_in_dim(
        cost_first, lax.axis_index("scen") * share_cols, share_cols, 0
    )
    first_weight = 1.0
    start_rows = starts[None]

    def couple(partial_value):
        return lax.psum_scatter(partial_value, "scen", scatter_dimension=1, tiled=True)

    def adjoint(rows_bf):
        first_part = jnp.dot(
            rows_bf.reshape(batch, scen_local * rows), tech_flat, preferred_element_type=f32
        )
        second_part = jnp.einsum("bsm,smk->bsk", rows_bf, recourse, preferred_element_type=f32)
        return (first_part, second_part)

    def local_squares(first_vec, second_vec):
        return first_weight * jnp.sum(first_vec * first_vec, axis=1) + jnp.sum(
            second_vec * second_vec, axis=(1, 2)
        )

    def total_norm(first_vec, second_vec):
        return lax.psum(local_squares(first_vec, second_vec), ("scen", "col"))

    here_rows = rhs.shape[2]
    first_sol = jnp.zeros((batch, share_cols), f32)
    second_sol = jnp.zeros((batch, scen_local, recourse.shape[2]), f32)
    slack = jnp.zeros((batch, scen_local, here_rows), f32)
    dual = jnp.zeros((batch, scen_local, here_rows), f32)
    image = jnp.zeros((batch, scen_local, here_rows), f32)
    for outer in range(ITERS):
        resid_rows = (rhs - slack - dual - image).astype(bf16)
        back_first, back_second = adjoint(resid_rows)
        res_first = couple(back_first) - cost_here[None, :]
        res_second = back_second - cost_second[None]
        res_norm = total_norm(res_first, res_second)
        dir_first, dir_second = (res_first, res_second)
        for step in range(CG_STEPS):
            dir_first_bf = lax.all_gather(dir_first.astype(bf16), "scen", axis=1, tiled=True)
            forward_partial_value = lax.dot_general(
                dir_first_bf, tech_flat, (((1,), (1,)), ((), ())), preferred_element_type=f32
            )
            forward_partial_value = forward_partial_value.reshape(batch, scen_local, rows)
            image_step = lax.psum(
                forward_partial_value
                + jnp.einsum(
                    "bsk,smk->bsm", dir_second.astype(bf16), recourse, preferred_element_type=f32
                ),
                "col",
            )
            curv_term = local_squares(dir_first, dir_second) + row_weight * jnp.sum(
                image_step * image_step, axis=(1, 2)
            )
            curv = lax.psum(curv_term, ("scen", "col"))
            alpha = res_norm / curv
            first_sol = first_sol + alpha[:, None] * dir_first
            second_sol = second_sol + alpha[:, None, None] * dir_second
            image = image + alpha[:, None, None] * image_step
            if step + 1 < CG_STEPS:
                back_first, back_second = adjoint(image_step.astype(bf16))
                res_first = res_first - alpha[:, None] * (dir_first + couple(back_first))
                res_second = res_second - alpha[:, None, None] * (dir_second + back_second)
                new_norm = total_norm(res_first, res_second)
                ratio = new_norm / res_norm
                dir_first = res_first + ratio[:, None] * dir_first
                dir_second = res_second + ratio[:, None, None] * dir_second
                res_norm = new_norm
        values = rhs - image - dual
        project_lead = jnp.einsum("bsm,smc->bsc", values * start_rows, onehot, precision=HIGH)
        project_tail = jnp.einsum(
            "bsm,smc->bsc", values * values * (1.0 - start_rows), onehot, precision=HIGH
        )
        project_lead, project_tail = (project_lead, project_tail)
        head, scale = cone_factors(project_lead, project_tail)
        head_rows = jnp.einsum("bsc,smc->bsm", head, onehot, precision=HIGH)
        scale_rows = jnp.einsum("bsc,smc->bsm", scale, onehot, precision=HIGH)
        slack = start_rows * head_rows + (1.0 - start_rows) * values * scale_rows
        dual = dual + image + slack - rhs
    first_out = lax.all_gather(first_sol, "scen", axis=1, tiled=True)
    slack_out = lax.dynamic_slice_in_dim(slack, row_start, part_rows, 2)
    dual_out = lax.dynamic_slice_in_dim(dual, row_start, part_rows, 2)
    return (first_out, second_sol, slack_out, dual_out)


def kernel_body(
    dims,
    tech_hbm, rec_hbm, rhs_hbm, cost1, cost2, cid, starts,
    x_out, y_out, slack_out, dual_out,
    tech, rec, g, dual, slack, onehot, q_all, part, rsc, q_own,
    acc, rs1, ag1, back2, res2, dir2, res1, dir1,
    nrm_own, nrm1, nrm_mid, nrm2, crv_own, crv1, crv_mid, crv2,
    nres, ratio, alpha, qq, xs,
    ld_t, ld_r, ld_g,
    ag1_s, ag1_r, n1_s, n1_r, n2_s, n2_r, rsc_s, rsc_r, agc_s, agc_r,
    c1_s, c1_r, c2_s, c2_r, rs1_s, rs1_r, fin_s, fin_r,
):
    n_scen, n_col, B, S, R, C1, C2 = dims
    f32, bf16 = jnp.float32, jnp.bfloat16
    RQ = R // n_col
    SH = C1 // n_scen
    G = B // 8
    W = 128 // G
    LAG = min(2, S)
    ms = lax.axis_index("scen")
    mc = lax.axis_index("col")

    def scen_peer(j):
        return lax.rem(ms + j, n_scen)

    def col_peer(j):
        return lax.rem(mc + j, n_col)

    def to_scen(src, dst, ss, rs, j):
        return pltpu.make_async_remote_copy(
            src_ref=src, dst_ref=dst, send_sem=ss, recv_sem=rs,
            device_id=(scen_peer(j), mc), device_id_type=pl.DeviceIdType.MESH)

    def to_col(src, dst, ss, rs, j):
        return pltpu.make_async_remote_copy(
            src_ref=src, dst_ref=dst, send_sem=ss, recv_sem=rs,
            device_id=(ms, col_peer(j)), device_id_type=pl.DeviceIdType.MESH)

    SJ = range(1, n_scen)
    CJ = range(1, n_col)

    def d_ag1(j):
        return to_scen(ag1.at[ms], ag1.at[ms], ag1_s.at[j - 1], ag1_r.at[j - 1], j)

    def d_n1(j):
        return to_scen(nrm_own, nrm1.at[j - 1], n1_s.at[j - 1], n1_r.at[j - 1], j)

    def d_n2(j):
        return to_col(nrm_mid, nrm2.at[j - 1], n2_s.at[j - 1], n2_r.at[j - 1], j)

    def d_rsc(j, s):
        return to_col(part.at[s, col_peer(j)], rsc.at[j - 1, s], rsc_s.at[j - 1, s], rsc_r.at[j - 1, s], j)

    def d_agc(j, s):
        return to_col(q_all.at[s, mc], q_all.at[s, mc], agc_s.at[j - 1, s], agc_r.at[j - 1, s], j)

    def d_c1(j):
        return to_col(crv_own, crv1.at[j - 1], c1_s.at[j - 1], c1_r.at[j - 1], j)

    def d_c2(j):
        return to_scen(crv_mid, crv2.at[j - 1], c2_s.at[j - 1], c2_r.at[j - 1], j)

    def d_rs1(j):
        return to_scen(acc.at[scen_peer(j)], rs1.at[j - 1], rs1_s.at[j - 1], rs1_r.at[j - 1], j)

    def d_fin(j):
        return to_scen(xs.at[ms], xs.at[ms], fin_s.at[j - 1], fin_r.at[j - 1], j)

    group = lax.broadcasted_iota(jnp.int32, (8, 128), 1) // W

    def pack(x):
        shift = 64
        while shift >= W:
            x = x + pltpu.roll(x, shift, 1)
            shift //= 2
        out = x[0:8]
        for k in range(1, G):
            out = jnp.where(group == k, x[8 * k:8 * k + 8], out)
        return out

    def unpack(p):
        return jnp.concatenate(
            [jnp.broadcast_to(jnp.sum(jnp.where(group == k, p, 0.0), axis=1, keepdims=True), (8, 128))
             for k in range(G)], axis=0)

    def lanes(x):
        out = x[:, 0:128]
        for k in range(1, x.shape[1] // 128):
            out = out + x[:, 128 * k:128 * k + 128]
        return out

    def load_t(s):
        return pltpu.make_async_copy(tech_hbm.at[s], tech.at[s], ld_t.at[s])

    def load_r(s):
        return pltpu.make_async_copy(rec_hbm.at[s], rec.at[s], ld_r.at[s])

    load_g = pltpu.make_async_copy(rhs_hbm, g, ld_g)
    load_g.start()
    for s in range(S):
        load_t(s).start()
        load_r(s).start()

    barrier = pltpu.get_barrier_semaphore()
    for j in SJ:
        pl.semaphore_signal(barrier, inc=1, device_id=(scen_peer(j), mc), device_id_type=pl.DeviceIdType.MESH)
    for j in CJ:
        pl.semaphore_signal(barrier, inc=1, device_id=(ms, col_peer(j)), device_id_type=pl.DeviceIdType.MESH)

    dir1[...] = jnp.zeros_like(dir1)
    dir2[...] = jnp.zeros_like(dir2)
    q_own[...] = jnp.zeros_like(q_own)
    dual[...] = jnp.zeros_like(dual)
    xs[ms] = jnp.zeros((B, SH), f32)
    y_out[...] = jnp.zeros_like(y_out)
    load_g.wait()

    def init(s, c):
        ids = cid[s]
        onehot[s] = (lax.broadcasted_iota(jnp.int32, (NCONE, R), 0) == ids).astype(f32).astype(bf16)
        for k in range(n_col):
            q_all[s, k] = g[s, :, k * RQ:(k + 1) * RQ].astype(bf16)
        return c

    lax.fori_loop(0, S, init, 0)
    pl.semaphore_wait(barrier, n_scen + n_col - 2)

    def curv_forward():
        total = crv_own[...]
        for j in CJ:
            d_c1(j).wait_recv()
            total = total + crv1[j - 1]
        for j in CJ:
            d_c1(j).wait_send()
        crv_mid[...] = total
        for j in SJ:
            d_c2(j).start()

    def curv_finish():
        total = crv_mid[...]
        for j in SJ:
            d_c2(j).wait_recv()
            total = total + crv2[j - 1]
        for j in SJ:
            d_c2(j).wait_send()
        alpha[...] = nres[...] / unpack(total)

    def advance():
        a = alpha[...][:, 0:1]
        xs[ms] = xs[ms] + a * dir1[...]

        def one(s, c):
            y_out[s] = y_out[s] + a * dir2[s]
            for k in range(n_col):
                cols = slice(k * RQ, (k + 1) * RQ)
                g[s, :, cols] = g[s, :, cols] - a * q_all[s, k].astype(f32)
            return c

        lax.fori_loop(0, S, one, 0)

    def split(x):
        hi = x.astype(bf16)
        return [hi, (x - hi.astype(f32)).astype(bf16)]

    def project(s, c):
        st = starts[s]
        v = g[s] - dual[s]
        lead_v = v * st
        tail_v = v * v * (1.0 - st)
        stack = jnp.concatenate(split(lead_v) + split(tail_v), axis=0)
        sums = lax.dot_general(stack, onehot[s], (((1,), (1,)), ((), ())), preferred_element_type=f32)
        lead = sums[0:B] + sums[B:2 * B]
        tail = sums[2 * B:3 * B] + sums[3 * B:4 * B]
        head, scale = cone_factors(lead, tail)
        stack2 = jnp.concatenate(split(head) + split(scale), axis=0)
        outs = jnp.dot(stack2, onehot[s], preferred_element_type=f32)
        head_rows = outs[0:B] + outs[B:2 * B]
        scale_rows = outs[2 * B:3 * B] + outs[3 * B:4 * B]
        sl = st * head_rows + (1.0 - st) * v * scale_rows
        du = sl - v
        slack[s] = sl
        dual[s] = du
        d = g[s] - sl - du
        for k in range(n_col):
            q_all[s, k] = d[:, k * RQ:(k + 1) * RQ].astype(bf16)
        return c

    def step_body(t, carry):
        step = lax.rem(t, CG_STEPS)
        acc[...] = jnp.zeros_like(acc)

        def back(s, c):
            @pl.when(t == 0)
            def _():
                load_t(s).wait()
                load_r(s).wait()

            @pl.when(step != 0)
            def _():
                for j in CJ:
                    d_agc(j, s).wait_recv()
                for j in CJ:
                    d_agc(j, s).wait_send()

            z = jnp.concatenate([q_all[s, k] for k in range(n_col)], axis=1)
            f = jnp.dot(z, tech[s], preferred_element_type=f32)
            for i in range(n_scen):
                acc[i] = acc[i] + f[:, i * SH:(i + 1) * SH]
            back2[s] = jnp.dot(z, rec[s], preferred_element_type=f32)

            @pl.when(jnp.logical_and(step != 0, s == S - 1))
            def _():
                curv_forward()

            return c

        lax.fori_loop(0, S, back, 0)
        for j in SJ:
            d_rs1(j).start()

        @pl.when(step != 0)
        def _():
            curv_finish()

        tot = acc[ms]
        for j in SJ:
            d_rs1(j).wait_recv()
            tot = tot + rs1[j - 1]
        for j in SJ:
            d_rs1(j).wait_send()

        @pl.when(step == 0)
        def _():
            res1[...] = tot - cost1[:, pl.ds(pl.multiple_of(ms * SH, 128), SH)]
            for s in range(S):
                res2[s] = back2[s] - cost2[s]

        @pl.when(step != 0)
        def _():
            a = alpha[...][:, 0:1]
            res1[...] = res1[...] - a * (dir1[...] + tot)
            for s in range(S):
                res2[s] = res2[s] - a * (dir2[s] + back2[s])

        r1 = res1[...]
        ag1[ms] = r1.astype(bf16)
        for j in SJ:
            d_ag1(j).start()
        sq = lanes(r1 * r1)
        for s in range(S):
            r2 = res2[s]
            sq = sq + lanes(r2 * r2)
        nrm_own[...] = pack(sq)
        for j in SJ:
            d_n1(j).start()

        @pl.when(step != 0)
        def _():
            advance()

        for j in SJ:
            d_ag1(j).wait_recv()
        for j in SJ:
            d_ag1(j).wait_send()

        def norm_forward():
            total = nrm_own[...]
            for j in SJ:
                d_n1(j).wait_recv()
                total = total + nrm1[j - 1]
            for j in SJ:
                d_n1(j).wait_send()
            nrm_mid[...] = total
            for j in CJ:
                d_n2(j).start()

        def norm_finish():
            total = nrm_mid[...]
            for j in CJ:
                d_n2(j).wait_recv()
                total = total + nrm2[j - 1]
            for j in CJ:
                d_n2(j).wait_send()
            new = unpack(total)

            @pl.when(step == 0)
            def _():
                ratio[...] = jnp.zeros_like(ratio)

            @pl.when(step != 0)
            def _():
                ratio[...] = new / nres[...]

            nres[...] = new
            r = ratio[...][:, 0:1]
            d1 = res1[...] + r * dir1[...]
            dir1[...] = d1
            dsq = lanes(d1 * d1)
            for s in range(S):
                d2 = res2[s] + r * dir2[s]
                dir2[s] = d2
                dsq = dsq + lanes(d2 * d2)
            qq[...] = dsq

        def process(s):
            r = ratio[...][:, 0:1]
            q = part[s, mc].astype(f32)
            for j in CJ:
                d_rsc(j, s).wait_recv()
                q = q + rsc[j - 1, s].astype(f32)
            q = q + r * q_own[s]
            q_own[s] = q
            q_all[s, mc] = q.astype(bf16)
            for j in CJ:
                d_agc(j, s).start()
            qq[...] = qq[...] + lanes(q * q)

        def front(s, c):
            x = jnp.concatenate([ag1[i] for i in range(n_scen)], axis=1)
            y = res2[s].astype(bf16)
            dn = (((1,), (1,)), ((), ()))
            for k in range(n_col):
                rows = pl.ds(k * RQ, RQ)
                p = lax.dot_general(x, tech[s, rows, :], dn, preferred_element_type=f32)
                p = p + lax.dot_general(y, rec[s, rows, :], dn, preferred_element_type=f32)
                part[s, k] = p.astype(bf16)
            for j in CJ:
                d_rsc(j, s).start()

            @pl.when(s == 0)
            def _():
                norm_forward()

            @pl.when(s == LAG - 1)
            def _():
                norm_finish()

            @pl.when(s >= LAG)
            def _():
                process(s - LAG)

            return c

        lax.fori_loop(0, S, front, 0)

        def drain(s, c):
            process(s)
            return c

        lax.fori_loop(S - LAG, S, drain, 0)
        crv_own[...] = pack(qq[...])
        for j in CJ:
            d_c1(j).start()
        for s in range(S):
            for j in CJ:
                d_rsc(j, s).wait_send()

        @pl.when(step == CG_STEPS - 1)
        def _():
            curv_forward()

            def arrive(s, c):
                for j in CJ:
                    d_agc(j, s).wait_recv()
                for j in CJ:
                    d_agc(j, s).wait_send()
                return c

            lax.fori_loop(0, S, arrive, 0)
            curv_finish()
            advance()
            lax.fori_loop(0, S, project, 0)

        return carry

    lax.fori_loop(0, ITERS * CG_STEPS, step_body, 0)

    for j in SJ:
        d_fin(j).start()
    here = pl.ds(pl.multiple_of(mc * RQ, 128), RQ)
    for s in range(S):
        slack_out[s] = slack[s, :, here]
        dual_out[s] = dual[s, :, here]
    for j in SJ:
        d_fin(j).wait_recv()
    for j in SJ:
        d_fin(j).wait_send()
    for i in range(n_scen):
        x_out[:, i * SH:(i + 1) * SH] = xs[i]


def fused(tech, recourse, rhs, cost_first, cost_second, cone_id):
    f32, bf16 = jnp.float32, jnp.bfloat16
    n_scen = lax.axis_size("scen")
    n_col = lax.axis_size("col")
    B = rhs.shape[0]
    S, R, C1 = tech.shape
    C2 = recourse.shape[2]
    RQ = R // n_col
    SH = C1 // n_scen
    starts = jnp.concatenate(
        [jnp.ones((S, 1), f32), (cone_id[:, 1:] != cone_id[:, :-1]).astype(f32)], axis=1)
    vm = pl.BlockSpec(memory_space=pltpu.VMEM)
    hbm = pl.BlockSpec(memory_space=pl.ANY)
    V = pltpu.VMEM
    D = pltpu.SemaphoreType.DMA
    ns, nc = n_scen - 1, n_col - 1
    scratch = [
        V((S, R, C1), bf16), V((S, R, C2), bf16),
        V((S, B, R), f32), V((S, B, R), f32), V((S, B, R), f32),
        V((S, NCONE, R), bf16),
        V((S, n_col, B, RQ), bf16), V((S, n_col, B, RQ), bf16), V((nc, S, B, RQ), bf16),
        V((S, B, RQ), f32),
        V((n_scen, B, SH), f32), V((ns, B, SH), f32), V((n_scen, B, SH), bf16),
        V((S, B, C2), f32), V((S, B, C2), f32), V((S, B, C2), f32),
        V((B, SH), f32), V((B, SH), f32),
        V((8, 128), f32), V((ns, 8, 128), f32), V((8, 128), f32), V((nc, 8, 128), f32),
        V((8, 128), f32), V((nc, 8, 128), f32), V((8, 128), f32), V((ns, 8, 128), f32),
        V((B, 128), f32), V((B, 128), f32), V((B, 128), f32), V((B, 128), f32),
        V((n_scen, B, SH), f32),
        D((S,)), D((S,)), D,
        D((ns,)), D((ns,)), D((ns,)), D((ns,)), D((nc,)), D((nc,)),
        D((nc, S)), D((nc, S)), D((nc, S)), D((nc, S)),
        D((nc,)), D((nc,)), D((ns,)), D((ns,)), D((ns,)), D((ns,)), D((ns,)), D((ns,)),
    ]
    x, y, slack, dual = pl.pallas_call(
        functools.partial(kernel_body, (n_scen, n_col, B, S, R, C1, C2)),
        out_shape=(
            jax.ShapeDtypeStruct((B, C1), f32),
            jax.ShapeDtypeStruct((S, B, C2), f32),
            jax.ShapeDtypeStruct((S, B, RQ), f32),
            jax.ShapeDtypeStruct((S, B, RQ), f32),
        ),
        in_specs=[hbm, hbm, hbm, vm, vm, vm, vm],
        out_specs=(vm, vm, vm, vm),
        scratch_shapes=scratch,
        compiler_params=pltpu.CompilerParams(
            collective_id=0, has_side_effects=True, vmem_limit_bytes=58 * 1024 * 1024),
    )(
        tech, recourse, jnp.transpose(rhs, (1, 0, 2)),
        cost_first.reshape(1, C1), cost_second.reshape(S, 1, C2),
        cone_id.reshape(S, 1, R), starts.reshape(S, 1, R),
    )
    back = lambda a: jnp.transpose(a, (1, 0, 2))
    return x, back(y), back(slack), back(dual)


def program(tech, recourse, rhs, cost_first, cost_second, cone_id):
    n_scen = lax.axis_size("scen")
    n_col = lax.axis_size("col")
    batch = rhs.shape[0]
    fits = (
        tech.shape[2] % (128 * n_scen) == 0
        and tech.shape[1] % (128 * n_col) == 0
        and recourse.shape[2] % 128 == 0
        and batch % 16 == 0
        and 1024 % batch == 0
        and n_scen > 1
        and n_col > 1
    )
    run = fused if fits else body
    return run(tech, recourse, rhs, cost_first, cost_second, cone_id)


def solution(mesh):
    placed = (
        P("scen", None, "col"),
        P("scen", None, "col"),
        P(None, "scen", None),
        P("col"),
        P("scen", "col"),
        P("scen", None),
    )
    return jax.shard_map(
        program,
        mesh=mesh,
        in_specs=placed,
        out_specs=(
            P(None, "col"),
            P(None, "scen", "col"),
            P(None, "scen", "col"),
            P(None, "scen", "col"),
        ),
        check_vma=False,
    )
```

```python
import functools

import jax
import jax.numpy as jnp
from jax import lax
from jax.experimental import pallas as pl
from jax.experimental.pallas import tpu as pltpu
from jax.sharding import PartitionSpec as P

NCONE = 128
ITERS = 3
CG_STEPS = 3


HIGH = lax.Precision.HIGHEST


def cone_factors(lead, tail):
    norm_tail = jnp.sqrt(tail)
    inside = norm_tail <= lead
    polar = norm_tail <= -lead
    safe = jnp.where(norm_tail > 0.0, norm_tail, 1.0)
    middle = 0.5 * (lead + norm_tail)
    head = jnp.where(inside, lead, jnp.where(polar, 0.0, middle))
    scale = jnp.where(inside, 1.0, jnp.where(polar, 0.0, middle / safe))
    return (head, scale)


def body(tech, recourse, rhs, cost_first, cost_second, cone_id):
    f32 = jnp.float32
    bf16 = jnp.bfloat16
    n_scen = lax.axis_size("scen")
    n_col = lax.axis_size("col")
    batch = rhs.shape[0]
    scen_local = tech.shape[0]
    rows = tech.shape[1]
    first_cols = tech.shape[2]
    tech_flat = tech.reshape(scen_local * rows, first_cols)
    starts = jnp.concatenate(
        [jnp.ones((scen_local, 1), f32), (cone_id[:, 1:] != cone_id[:, :-1]).astype(f32)], axis=1
    )
    labels = lax.broadcasted_iota(jnp.int32, (1, 1, NCONE), 2)
    onehot = (cone_id[:, :, None] == labels).astype(f32)
    part_rows = rows // n_col
    row_start = lax.axis_index("col") * part_rows
    row_weight = 1.0 / n_col
    share_cols = first_cols // n_scen
    cost_here = lax.dynamic_slice_in_dim(
        cost_first, lax.axis_index("scen") * share_cols, share_cols, 0
    )
    first_weight = 1.0
    start_rows = starts[None]

    def couple(partial_value):
        return lax.psum_scatter(partial_value, "scen", scatter_dimension=1, tiled=True)

    def adjoint(rows_bf):
        first_part = jnp.dot(
            rows_bf.reshape(batch, scen_local * rows), tech_flat, preferred_element_type=f32
        )
        second_part = jnp.einsum("bsm,smk->bsk", rows_bf, recourse, preferred_element_type=f32)
        return (first_part, second_part)

    def local_squares(first_vec, second_vec):
        return first_weight * jnp.sum(first_vec * first_vec, axis=1) + jnp.sum(
            second_vec * second_vec, axis=(1, 2)
        )

    def total_norm(first_vec, second_vec):
        return lax.psum(local_squares(first_vec, second_vec), ("scen", "col"))

    here_rows = rhs.shape[2]
    first_sol = jnp.zeros((batch, share_cols), f32)
    second_sol = jnp.zeros((batch, scen_local, recourse.shape[2]), f32)
    slack = jnp.zeros((batch, scen_local, here_rows), f32)
    dual = jnp.zeros((batch, scen_local, here_rows), f32)
    image = jnp.zeros((batch, scen_local, here_rows), f32)
    for outer in range(ITERS):
        resid_rows = (rhs - slack - dual - image).astype(bf16)
        back_first, back_second = adjoint(resid_rows)
        res_first = couple(back_first) - cost_here[None, :]
        res_second = back_second - cost_second[None]
        res_norm = total_norm(res_first, res_second)
        dir_first, dir_second = (res_first, res_second)
        for step in range(CG_STEPS):
            dir_first_bf = lax.all_gather(dir_first.astype(bf16), "scen", axis=1, tiled=True)
            forward_partial_value = lax.dot_general(
                dir_first_bf, tech_flat, (((1,), (1,)), ((), ())), preferred_element_type=f32
            )
            forward_partial_value = forward_partial_value.reshape(batch, scen_local, rows)
            image_step = lax.psum(
                forward_partial_value
                + jnp.einsum(
                    "bsk,smk->bsm", dir_second.astype(bf16), recourse, preferred_element_type=f32
                ),
                "col",
            )
            curv_term = local_squares(dir_first, dir_second) + row_weight * jnp.sum(
                image_step * image_step, axis=(1, 2)
            )
            curv = lax.psum(curv_term, ("scen", "col"))
            alpha = res_norm / curv
            first_sol = first_sol + alpha[:, None] * dir_first
            second_sol = second_sol + alpha[:, None, None] * dir_second
            image = image + alpha[:, None, None] * image_step
            if step + 1 < CG_STEPS:
                back_first, back_second = adjoint(image_step.astype(bf16))
                res_first = res_first - alpha[:, None] * (dir_first + couple(back_first))
                res_second = res_second - alpha[:, None, None] * (dir_second + back_second)
                new_norm = total_norm(res_first, res_second)
                ratio = new_norm / res_norm
                dir_first = res_first + ratio[:, None] * dir_first
                dir_second = res_second + ratio[:, None, None] * dir_second
                res_norm = new_norm
        values = rhs - image - dual
        project_lead = jnp.einsum("bsm,smc->bsc", values * start_rows, onehot, precision=HIGH)
        project_tail = jnp.einsum(
            "bsm,smc->bsc", values * values * (1.0 - start_rows), onehot, precision=HIGH
        )
        project_lead, project_tail = (project_lead, project_tail)
        head, scale = cone_factors(project_lead, project_tail)
        head_rows = jnp.einsum("bsc,smc->bsm", head, onehot, precision=HIGH)
        scale_rows = jnp.einsum("bsc,smc->bsm", scale, onehot, precision=HIGH)
        slack = start_rows * head_rows + (1.0 - start_rows) * values * scale_rows
        dual = dual + image + slack - rhs
    first_out = lax.all_gather(first_sol, "scen", axis=1, tiled=True)
    slack_out = lax.dynamic_slice_in_dim(slack, row_start, part_rows, 2)
    dual_out = lax.dynamic_slice_in_dim(dual, row_start, part_rows, 2)
    return (first_out, second_sol, slack_out, dual_out)


def kernel_body(
    dims,
    tech_hbm, rec_hbm, rhs_hbm, cost1, cost2, cid, starts,
    x_out, y_out, slack_out, dual_out,
    tech, rec, g, dual, slack, onehot, q_all, part, rsc, q_own,
    acc, snd, rs1, ag1, back2, res2, dir2, res1, dir1,
    nrm_own, nrm1, nrm_mid, nrm2, crv_own, crv1, crv_mid, crv2,
    nres, ratio, alpha, qq, xs,
    ld_t, ld_r, ld_g,
    ag1_s, ag1_r, n1_s, n1_r, n2_s, n2_r, rsc_s, rsc_r, agc_s, agc_r,
    c1_s, c1_r, c2_s, c2_r, rs1_s, rs1_r, fin_s, fin_r,
):
    n_scen, n_col, B, S, R, C1, C2 = dims
    f32, bf16 = jnp.float32, jnp.bfloat16
    RQ = R // n_col
    SH = C1 // n_scen
    G = B // 8
    W = 128 // G
    ms = lax.axis_index("scen")
    mc = lax.axis_index("col")

    def scen_peer(j):
        return lax.rem(ms + j, n_scen)

    def col_peer(j):
        return lax.rem(mc + j, n_col)

    def to_scen(src, dst, ss, rs, j):
        return pltpu.make_async_remote_copy(
            src_ref=src, dst_ref=dst, send_sem=ss, recv_sem=rs,
            device_id=(scen_peer(j), mc), device_id_type=pl.DeviceIdType.MESH)

    def to_col(src, dst, ss, rs, j):
        return pltpu.make_async_remote_copy(
            src_ref=src, dst_ref=dst, send_sem=ss, recv_sem=rs,
            device_id=(ms, col_peer(j)), device_id_type=pl.DeviceIdType.MESH)

    SJ = range(1, n_scen)
    CJ = range(1, n_col)

    def d_ag1(j):
        return to_scen(ag1.at[ms], ag1.at[ms], ag1_s.at[j - 1], ag1_r.at[j - 1], j)

    def d_n1(j):
        return to_scen(nrm_own, nrm1.at[j - 1], n1_s.at[j - 1], n1_r.at[j - 1], j)

    def d_n2(j):
        return to_col(nrm_mid, nrm2.at[j - 1], n2_s.at[j - 1], n2_r.at[j - 1], j)

    def d_rsc(j, s):
        return to_col(part.at[s, col_peer(j)], rsc.at[j - 1, s], rsc_s.at[j - 1, s], rsc_r.at[j - 1, s], j)

    def d_agc(j, s):
        return to_col(q_all.at[s, mc], q_all.at[s, mc], agc_s.at[j - 1, s], agc_r.at[j - 1, s], j)

    def d_c1(j):
        return to_col(crv_own, crv1.at[j - 1], c1_s.at[j - 1], c1_r.at[j - 1], j)

    def d_c2(j):
        return to_scen(crv_mid, crv2.at[j - 1], c2_s.at[j - 1], c2_r.at[j - 1], j)

    def d_rs1(j):
        return to_scen(snd.at[scen_peer(j)], rs1.at[j - 1], rs1_s.at[j - 1], rs1_r.at[j - 1], j)

    def d_fin(j):
        return to_scen(xs.at[ms], xs.at[ms], fin_s.at[j - 1], fin_r.at[j - 1], j)

    group = lax.broadcasted_iota(jnp.int32, (8, 128), 1) // W

    def pack(x):
        shift = 64
        while shift >= W:
            x = x + pltpu.roll(x, shift, 1)
            shift //= 2
        out = x[0:8]
        for k in range(1, G):
            out = jnp.where(group == k, x[8 * k:8 * k + 8], out)
        return out

    def unpack(p):
        return jnp.concatenate(
            [jnp.broadcast_to(jnp.sum(jnp.where(group == k, p, 0.0), axis=1, keepdims=True), (8, 128))
             for k in range(G)], axis=0)

    def lanes(x):
        out = x[:, 0:128]
        for k in range(1, x.shape[1] // 128):
            out = out + x[:, 128 * k:128 * k + 128]
        return out

    def load_t(s):
        return pltpu.make_async_copy(tech_hbm.at[s], tech.at[s], ld_t.at[s])

    def load_r(s):
        return pltpu.make_async_copy(rec_hbm.at[s], rec.at[s], ld_r.at[s])

    load_g = pltpu.make_async_copy(rhs_hbm, g, ld_g)
    load_g.start()
    for s in range(S):
        load_t(s).start()
        load_r(s).start()

    barrier = pltpu.get_barrier_semaphore()
    for j in SJ:
        pl.semaphore_signal(barrier, inc=1, device_id=(scen_peer(j), mc), device_id_type=pl.DeviceIdType.MESH)
    for j in CJ:
        pl.semaphore_signal(barrier, inc=1, device_id=(ms, col_peer(j)), device_id_type=pl.DeviceIdType.MESH)

    dir1[...] = jnp.zeros_like(dir1)
    dir2[...] = jnp.zeros_like(dir2)
    q_own[...] = jnp.zeros_like(q_own)
    dual[...] = jnp.zeros_like(dual)
    xs[ms] = jnp.zeros((B, SH), f32)
    y_out[...] = jnp.zeros_like(y_out)
    load_g.wait()

    def init(s, c):
        ids = cid[pl.ds(s, 1), :]
        onehot[s] = (lax.broadcasted_iota(jnp.int32, (NCONE, R), 0) == ids).astype(f32).astype(bf16)
        for k in range(n_col):
            q_all[s, k] = g[s, :, k * RQ:(k + 1) * RQ].astype(bf16)
        return c

    lax.fori_loop(0, S, init, 0)
    pl.semaphore_wait(barrier, n_scen + n_col - 2)

    def curv_forward():
        total = crv_own[...]
        for j in CJ:
            d_c1(j).wait_recv()
            total = total + crv1[j - 1]
        for j in CJ:
            d_c1(j).wait_send()
        crv_mid[...] = total
        for j in SJ:
            d_c2(j).start()

    def curv_finish():
        total = crv_mid[...]
        for j in SJ:
            d_c2(j).wait_recv()
            total = total + crv2[j - 1]
        for j in SJ:
            d_c2(j).wait_send()
        alpha[...] = nres[...] / unpack(total)

    def advance():
        a = alpha[...][:, 0:1]
        xs[ms] = xs[ms] + a * dir1[...]

        def one(s, c):
            y_out[s] = y_out[s] + a * dir2[s]
            for k in range(n_col):
                cols = slice(k * RQ, (k + 1) * RQ)
                g[s, :, cols] = g[s, :, cols] - a * q_all[s, k].astype(f32)
            return c

        lax.fori_loop(0, S, one, 0)

    def split(x):
        hi = x.astype(bf16)
        return [hi, (x - hi.astype(f32)).astype(bf16)]

    def project(s, c):
        st = starts[pl.ds(s, 1), :]
        v = g[s] - dual[s]
        lead_v = v * st
        tail_v = v * v * (1.0 - st)
        stack = jnp.concatenate(split(lead_v) + split(tail_v), axis=0)
        sums = lax.dot_general(stack, onehot[s], (((1,), (1,)), ((), ())), preferred_element_type=f32)
        lead = sums[0:B] + sums[B:2 * B]
        tail = sums[2 * B:3 * B] + sums[3 * B:4 * B]
        head, scale = cone_factors(lead, tail)
        stack2 = jnp.concatenate(split(head) + split(scale), axis=0)
        outs = jnp.dot(stack2, onehot[s], preferred_element_type=f32)
        head_rows = outs[0:B] + outs[B:2 * B]
        scale_rows = outs[2 * B:3 * B] + outs[3 * B:4 * B]
        sl = st * head_rows + (1.0 - st) * v * scale_rows
        du = sl - v
        slack[s] = sl
        dual[s] = du
        d = g[s] - sl - du
        for k in range(n_col):
            q_all[s, k] = d[:, k * RQ:(k + 1) * RQ].astype(bf16)
        return c

    def step_body(t, carry):
        step = lax.rem(t, CG_STEPS)
        acc[...] = jnp.zeros_like(acc)

        def back(s, c):
            @pl.when(t == 0)
            def _():
                load_t(s).wait()
                load_r(s).wait()

            @pl.when(step != 0)
            def _():
                for j in CJ:
                    d_agc(j, s).wait_recv()
                for j in CJ:
                    d_agc(j, s).wait_send()

            z = jnp.concatenate([q_all[s, k] for k in range(n_col)], axis=1)
            f = jnp.dot(z, tech[s], preferred_element_type=f32)
            for i in range(n_scen):
                acc[i] = acc[i] + f[:, i * SH:(i + 1) * SH]
            back2[s] = jnp.dot(z, rec[s], preferred_element_type=f32)

            @pl.when(jnp.logical_and(step != 0, s == S - 1))
            def _():
                curv_forward()

            return c

        lax.fori_loop(0, S, back, 0)
        for i in range(n_scen):
            snd[i] = acc[i].astype(bf16)
        for j in SJ:
            d_rs1(j).start()

        @pl.when(step != 0)
        def _():
            curv_finish()

        tot = acc[ms]
        for j in SJ:
            d_rs1(j).wait_recv()
            tot = tot + rs1[j - 1].astype(f32)
        for j in SJ:
            d_rs1(j).wait_send()

        @pl.when(step == 0)
        def _():
            res1[...] = tot - cost1[:, pl.ds(pl.multiple_of(ms * SH, 128), SH)]
            for s in range(S):
                res2[s] = back2[s] - cost2[s:s + 1, :]

        @pl.when(step != 0)
        def _():
            a = alpha[...][:, 0:1]
            res1[...] = res1[...] - a * (dir1[...] + tot)
            for s in range(S):
                res2[s] = res2[s] - a * (dir2[s] + back2[s])

        r1 = res1[...]
        ag1[ms] = r1.astype(bf16)
        for j in SJ:
            d_ag1(j).start()
        sq = lanes(r1 * r1)
        for s in range(S):
            r2 = res2[s]
            sq = sq + lanes(r2 * r2)
        nrm_own[...] = pack(sq)
        for j in SJ:
            d_n1(j).start()

        @pl.when(step != 0)
        def _():
            advance()

        for j in SJ:
            d_ag1(j).wait_recv()
        for j in SJ:
            d_ag1(j).wait_send()

        def norm_forward():
            total = nrm_own[...]
            for j in SJ:
                d_n1(j).wait_recv()
                total = total + nrm1[j - 1]
            for j in SJ:
                d_n1(j).wait_send()
            nrm_mid[...] = total
            for j in CJ:
                d_n2(j).start()

        def norm_finish():
            total = nrm_mid[...]
            for j in CJ:
                d_n2(j).wait_recv()
                total = total + nrm2[j - 1]
            for j in CJ:
                d_n2(j).wait_send()
            new = unpack(total)

            @pl.when(step == 0)
            def _():
                ratio[...] = jnp.zeros_like(ratio)

            @pl.when(step != 0)
            def _():
                ratio[...] = new / nres[...]

            nres[...] = new
            r = ratio[...][:, 0:1]
            d1 = res1[...] + r * dir1[...]
            dir1[...] = d1
            dsq = lanes(d1 * d1)
            for s in range(S):
                d2 = res2[s] + r * dir2[s]
                dir2[s] = d2
                dsq = dsq + lanes(d2 * d2)
            qq[...] = dsq

        def process(s):
            r = ratio[...][:, 0:1]
            q = part[s, mc].astype(f32)
            for j in CJ:
                d_rsc(j, s).wait_recv()
                q = q + rsc[j - 1, s].astype(f32)
            q = q + r * q_own[s]
            q_own[s] = q
            q_all[s, mc] = q.astype(bf16)
            for j in CJ:
                d_agc(j, s).start()
            qq[...] = qq[...] + lanes(q * q)

        def front(s, c):
            x = jnp.concatenate([ag1[i] for i in range(n_scen)], axis=1)
            y = res2[s].astype(bf16)
            dn = (((1,), (1,)), ((), ()))
            for k in range(n_col):
                rows = pl.ds(k * RQ, RQ)
                p = lax.dot_general(x, tech[s, rows, :], dn, preferred_element_type=f32)
                p = p + lax.dot_general(y, rec[s, rows, :], dn, preferred_element_type=f32)
                part[s, k] = p.astype(bf16)

            @pl.when(s == 0)
            def _():
                norm_forward()

            for j in CJ:
                d_rsc(j, s).start()
            return c

        lax.fori_loop(0, S, front, 0)
        norm_finish()

        def drain(s, c):
            process(s)
            return c

        lax.fori_loop(0, S, drain, 0)
        crv_own[...] = pack(qq[...])
        for j in CJ:
            d_c1(j).start()
        for s in range(S):
            for j in CJ:
                d_rsc(j, s).wait_send()

        @pl.when(step == CG_STEPS - 1)
        def _():
            curv_forward()

            def arrive(s, c):
                for j in CJ:
                    d_agc(j, s).wait_recv()
                for j in CJ:
                    d_agc(j, s).wait_send()
                return c

            lax.fori_loop(0, S, arrive, 0)
            curv_finish()
            advance()
            lax.fori_loop(0, S, project, 0)

        return carry

    lax.fori_loop(0, ITERS * CG_STEPS, step_body, 0)

    for j in SJ:
        d_fin(j).start()
    here = pl.ds(pl.multiple_of(mc * RQ, 128), RQ)
    for s in range(S):
        slack_out[s] = slack[s, :, here]
        dual_out[s] = dual[s, :, here]
    for j in SJ:
        d_fin(j).wait_recv()
    for j in SJ:
        d_fin(j).wait_send()
    for i in range(n_scen):
        x_out[:, i * SH:(i + 1) * SH] = xs[i]


def fused(tech, recourse, rhs, cost_first, cost_second, cone_id):
    f32, bf16 = jnp.float32, jnp.bfloat16
    n_scen = lax.axis_size("scen")
    n_col = lax.axis_size("col")
    B = rhs.shape[0]
    S, R, C1 = tech.shape
    C2 = recourse.shape[2]
    RQ = R // n_col
    SH = C1 // n_scen
    starts = jnp.concatenate(
        [jnp.ones((S, 1), f32), (cone_id[:, 1:] != cone_id[:, :-1]).astype(f32)], axis=1)
    vm = pl.BlockSpec(memory_space=pltpu.VMEM)
    hbm = pl.BlockSpec(memory_space=pl.ANY)
    V = pltpu.VMEM
    D = pltpu.SemaphoreType.DMA
    ns, nc = n_scen - 1, n_col - 1
    scratch = [
        V((S, R, C1), bf16), V((S, R, C2), bf16),
        V((S, B, R), f32), V((S, B, R), f32), V((S, B, R), f32),
        V((S, NCONE, R), bf16),
        V((S, n_col, B, RQ), bf16), V((S, n_col, B, RQ), bf16), V((nc, S, B, RQ), bf16),
        V((S, B, RQ), f32),
        V((n_scen, B, SH), f32), V((n_scen, B, SH), bf16), V((ns, B, SH), bf16), V((n_scen, B, SH), bf16),
        V((S, B, C2), f32), V((S, B, C2), f32), V((S, B, C2), f32),
        V((B, SH), f32), V((B, SH), f32),
        V((8, 128), f32), V((ns, 8, 128), f32), V((8, 128), f32), V((nc, 8, 128), f32),
        V((8, 128), f32), V((nc, 8, 128), f32), V((8, 128), f32), V((ns, 8, 128), f32),
        V((B, 128), f32), V((B, 128), f32), V((B, 128), f32), V((B, 128), f32),
        V((n_scen, B, SH), f32),
        D((S,)), D((S,)), D,
        D((ns,)), D((ns,)), D((ns,)), D((ns,)), D((nc,)), D((nc,)),
        D((nc, S)), D((nc, S)), D((nc, S)), D((nc, S)),
        D((nc,)), D((nc,)), D((ns,)), D((ns,)), D((ns,)), D((ns,)), D((ns,)), D((ns,)),
    ]
    x, y, slack, dual = pl.pallas_call(
        functools.partial(kernel_body, (n_scen, n_col, B, S, R, C1, C2)),
        out_shape=(
            jax.ShapeDtypeStruct((B, C1), f32),
            jax.ShapeDtypeStruct((S, B, C2), f32),
            jax.ShapeDtypeStruct((S, B, RQ), f32),
            jax.ShapeDtypeStruct((S, B, RQ), f32),
        ),
        in_specs=[hbm, hbm, hbm, vm, vm, vm, vm],
        out_specs=(vm, vm, vm, vm),
        scratch_shapes=scratch,
        compiler_params=pltpu.CompilerParams(
            collective_id=0, has_side_effects=True, vmem_limit_bytes=58 * 1024 * 1024),
    )(
        tech, recourse, jnp.transpose(rhs, (1, 0, 2)),
        cost_first.reshape(1, C1), cost_second, cone_id, starts,
    )
    back = lambda a: jnp.transpose(a, (1, 0, 2))
    return x, back(y), back(slack), back(dual)


def program(tech, recourse, rhs, cost_first, cost_second, cone_id):
    n_scen = lax.axis_size("scen")
    n_col = lax.axis_size("col")
    batch = rhs.shape[0]
    fits = (
        tech.shape[2] % (128 * n_scen) == 0
        and tech.shape[1] % (128 * n_col) == 0
        and recourse.shape[2] % 128 == 0
        and batch % 16 == 0
        and 1024 % batch == 0
        and n_scen > 1
        and n_col > 1
    )
    run = fused if fits else body
    return run(tech, recourse, rhs, cost_first, cost_second, cone_id)


def solution(mesh):
    placed = (
        P("scen", None, "col"),
        P("scen", None, "col"),
        P(None, "scen", None),
        P("col"),
        P("scen", "col"),
        P("scen", None),
    )
    return jax.shard_map(
        program,
        mesh=mesh,
        in_specs=placed,
        out_specs=(
            P(None, "col"),
            P(None, "scen", "col"),
            P(None, "scen", "col"),
            P(None, "scen", "col"),
        ),
        check_vma=False,
    )
```
